256 devices in a mesh: gy: 8 (over y, x_hi), gx: 32 (over x_lo, z, core).
Axes of the slice: x: 4 (x_hi: 2, x_lo: 2; x = x_hi * 2 + x_lo), y: 4, z: 8, core: 2. Of those that a mesh axis runs over, the one named last changes fastest.
Arguments:
- u_field: float32 [8, 2048, 2048], P(None, 'gx', 'gy')
- v_field: float32 [8, 2048, 2048], P(None, 'gx', 'gy')
- w_field: float32 [8, 2048, 2048], P(None, 'gx', 'gy')
- sep_x: int32 [16], replicated, may hold values from 1 to 128, as said below
- sep_y: int32 [16], replicated, may hold values from 1 to 256, as said below
- sep_z: int32 [16], replicated, may hold values from 1 to 4
Outputs:
- correlation: float32 [3, 16], replicated
The draws below stay inside these ranges and needn't reach their ends.
Inputs may be any that keep to these rules, and one draw needn't show every extreme that they name: `sep_x`: every separation along x lies in 1 to 128, and 128 is among them in every draw; repeats may occur. `sep_y`: every separation along y lies in 1 to 256, and 256 is among them in every draw; repeats may occur.
All inputs are finite; a program needn't handle non-finite values.
Results may differ from the reference program's by a relative error of at most 0.0003.
Values sent between devices are 32-bit elements; how exact they have to be, the bound alone decides.
A program may use at most 64 MiB of HBM per device.

```python
import math
import jax
import jax.numpy as jnp
from jax import lax

PLANES = 8
CX = 64
CY = 256
SEPS = 16
NX = 2048
NY = 2048


def rough_scale(key, shape, spread):
    return jnp.exp(jax.random.uniform(key, shape, jnp.float32, -spread, spread))


def smooth_field(key, salt_value):
    key = jax.random.fold_in(key, salt_value)
    key_list = jax.random.split(key, 12)
    mode_count = 6
    plane_pos = jnp.arange(PLANES, dtype=jnp.float32)[:, None, None]
    row_pos = jnp.arange(NX, dtype=jnp.float32)[None, :, None]
    column_pos = jnp.arange(NY, dtype=jnp.float32)[None, None, :]
    wave_x = jax.random.randint(key_list[0], (mode_count,), 1, 5).astype(jnp.float32)
    wave_y = jax.random.randint(key_list[1], (mode_count,), 1, 5).astype(jnp.float32)
    wave_z = jax.random.randint(key_list[2], (mode_count,), 0, 3).astype(jnp.float32)
    phases = jax.random.uniform(key_list[3], (mode_count, 3), jnp.float32, 0.0, 2.0 * math.pi)
    amplitude = jax.random.uniform(key_list[4], (mode_count,), jnp.float32, 0.5, 1.0)
    smooth = jnp.zeros((PLANES, NX, NY), jnp.float32)
    for mode_index in range(mode_count):
        cos_x = jnp.cos(2.0 * math.pi * wave_x[mode_index] * row_pos / NX + phases[mode_index, 0])
        cos_y = jnp.cos(2.0 * math.pi * wave_y[mode_index] * column_pos / NY + phases[mode_index, 1])
        cos_z = jnp.cos(2.0 * math.pi * wave_z[mode_index] * plane_pos / (4.0 * PLANES) + phases[mode_index, 2])
        smooth = smooth + amplitude[mode_index] * cos_x * cos_y * cos_z
    spread = 1.15
    noise_part = 0.7 * jax.random.normal(key_list[11], (PLANES, NX, NY), jnp.float32)
    smooth_scale = rough_scale(key_list[5], (PLANES, 1, 1), spread) * rough_scale(key_list[6], (1, NX, 1), spread) * rough_scale(key_list[7], (1, 1, NY), spread)
    noise_scale = rough_scale(key_list[8], (PLANES, 1, 1), spread) * rough_scale(key_list[9], (1, NX, 1), spread) * rough_scale(key_list[10], (1, 1, NY), spread)
    return smooth_scale * (1.5 * smooth) + noise_scale * noise_part


def draw_u_field(key, part):
    return smooth_field(key, 11)


def draw_v_field(key, part):
    return smooth_field(key, 23)


def draw_w_field(key, part):
    return smooth_field(key, 37)


def separations(key, salt_value, largest):
    key = jax.random.fold_in(key, salt_value)
    key_list = jax.random.split(key, 2)
    others = jax.random.randint(key_list[0], (SEPS - 1,), 1, largest + 1)
    values = jnp.concatenate([others, jnp.full((1,), largest, jnp.int32)])
    return jax.random.permutation(key_list[1], values).astype(jnp.int32)


def draw_sep_x(key, part):
    return separations(key, 41, 2 * CX)


def draw_sep_y(key, part):
    return separations(key, 53, CY)


def touch_ends(drawn, stream_key, smallest, top_value):
    dims = drawn.shape
    index_at = [jax.random.randint(jax.random.fold_in(stream_key, axis), (), 0, dims[axis]) for axis in range(len(dims))]
    drawn = drawn.at[tuple(index_at)].set(smallest)
    longest = dims.index(max(dims))
    index_at[longest] = (index_at[longest] + 1) % dims[longest]
    return drawn.at[tuple(index_at)].set(top_value)


def setup_inputs(seed: int = 0) -> dict:
    streams_of = jax.random.split(jax.random.key(seed), 7)
    u_field = draw_u_field(jax.random.fold_in(streams_of[6], 71), 0)
    v_field = draw_v_field(jax.random.fold_in(streams_of[6], 71), 0)
    w_field = draw_w_field(jax.random.fold_in(streams_of[6], 71), 0)
    sep_x = draw_sep_x(jax.random.fold_in(streams_of[6], 71), 0)
    sep_y = draw_sep_y(jax.random.fold_in(streams_of[6], 71), 0)
    sep_z = touch_ends(jax.random.randint(streams_of[5], (SEPS,), 1, PLANES // 2 + 1), jax.random.fold_in(streams_of[5], 1), 1, (PLANES // 2 + 1) - 1).astype(jnp.int32)
    return {"u_field": u_field, "v_field": v_field, "w_field": w_field, "sep_x": sep_x, "sep_y": sep_y, "sep_z": sep_z}


def reference(u_field, v_field, w_field, sep_x, sep_y, sep_z):
    planes = u_field.shape[0]

    def along_x(lag_value):
        return jnp.sum(u_field * jnp.roll(u_field, -lag_value, axis=1))

    def along_y(lag_value):
        return jnp.sum(v_field * jnp.roll(v_field, -lag_value, axis=2))

    padded = jnp.concatenate([w_field, jnp.zeros_like(w_field)], axis=0)

    def along_z(lag_value):
        shifted = lax.dynamic_slice_in_dim(padded, lag_value.astype(jnp.int32), planes, 0)
        return jnp.sum(w_field * shifted)

    sums_x = lax.map(along_x, sep_x)
    sums_y = lax.map(along_y, sep_y)
    sums_z = lax.map(along_z, sep_z)
    energy_u = jnp.sum(u_field * u_field)
    energy_v = jnp.sum(v_field * v_field)
    energy_w = jnp.sum(w_field * w_field)
    factor = jnp.float32(planes) / (jnp.float32(planes) - sep_z.astype(jnp.float32))
    row_x = sums_x / energy_u
    row_y = sums_y / energy_v
    row_z = sums_z / energy_w * factor
    return jnp.stack([row_x, row_y, row_z], axis=0)
```

```python
import functools

import jax
import jax.numpy as jnp
from jax import lax
from jax.experimental import pallas as pl
from jax.experimental.pallas import tpu as pltpu
from jax.sharding import PartitionSpec as P

F32 = jnp.float32
BF16 = jnp.bfloat16
MESH = pl.DeviceIdType.MESH
NT = (((1,), (1,)), ((), ()))
TN = (((0,), (0,)), ((), ()))


def place(x, y, z, core):
    return {"gy": y * 2 + x // 2, "gx": (x % 2) * 16 + z * 2 + core}


def split(value):
    high = value.astype(BF16)
    low = (value - high.astype(F32)).astype(BF16)
    return high, low


def gram(a, b, dims):
    dot = functools.partial(lax.dot_general, dimension_numbers=dims, preferred_element_type=F32)
    return dot(a[0], b[0]) + (dot(a[0], b[1]) + dot(a[1], b[0]))


def lag_row(block):
    total = block[0:8]
    for start in range(8, 128, 8):
        total += pltpu.roll(block[start:start + 8], 128 - start, 1)
    row = lax.broadcasted_iota(jnp.int32, (8, 128), 0)
    for bit in (1, 2, 4):
        total = jnp.where(row & bit != 0, pltpu.roll(total, 128 - bit, 1), total)
    return jnp.sum(total, axis=0, keepdims=True)


def kernel(u_hbm, v_hbm, w_hbm, sx_ref, sy_ref, sz_ref, out_ref,
           u_own, v_own, w_own, u_chip, u_near, v_pair, v_fwd, tile, got1, mid, got2,
           load_sem, send_sem, d2d_sem, u_sem, v_sem, y_sem, red_send, red_recv):
    gy = lax.axis_index("gy")
    gx = lax.axis_index("gx")
    y, x_hi = gy // 2, gy % 2
    x_lo, z, core = gx // 16, (gx // 2) % 8, gx % 2
    x = x_hi * 2 + x_lo
    ring = x_lo * 8 + z
    after, before = (ring + 1) % 16, (ring + 15) % 16

    def chip_u(pos, c):
        return {"gy": gy, "gx": pos * 2 + c}

    def group1(i):
        return {"gy": gy, "gx": x_lo * 16 + (gx % 16 + i) % 16}

    own2 = x * 4 + y

    def group2(i):
        other = (own2 + i) % 16
        return place(other // 4, other % 4, z, core)

    loads = [
        pltpu.make_async_copy(v_hbm, v_own, load_sem.at[0]),
        pltpu.make_async_copy(u_hbm, u_own, load_sem.at[1]),
        pltpu.make_async_copy(
            u_hbm.at[pl.ds(4 * core, 4)], u_chip.at[:, pl.ds(64 * core, 64), :], load_sem.at[2]),
        pltpu.make_async_copy(w_hbm, w_own, load_sem.at[3]),
    ]
    for load in loads:
        load.start()

    barrier = pltpu.get_barrier_semaphore()
    for pos in (after, before):
        for c in range(2):
            pl.semaphore_signal(barrier, inc=1, device_id=chip_u(pos, c), device_id_type=MESH)

    def greet(i, carry):
        pl.semaphore_signal(barrier, inc=1, device_id=group1(i), device_id_type=MESH)
        pl.semaphore_signal(barrier, inc=1, device_id=group2(i), device_id_type=MESH)
        return carry

    lax.fori_loop(1, 16, greet, 0)
    pl.semaphore_wait(barrier, 34)

    sends = []

    def send(src, dst, sem, target):
        copy = pltpu.make_async_remote_copy(
            src_ref=src, dst_ref=dst, send_sem=send_sem.at[len(sends)], recv_sem=sem,
            device_id=target, device_id_type=MESH)
        copy.start()
        sends.append(copy)

    loads[0].wait()
    for chunk in range(2):
        lead = (x_hi + chunk) % 2 * 2
        for step in (1, 3):
            other = (x + step) % 4
            base = ((other + 3) % 4) // 2 * 4
            send(v_own.at[pl.ds(base + lead, 2)], v_pair.at[x_hi, pl.ds(lead, 2)],
                 v_sem.at[x_hi, chunk], place(other, y, z, core))
    loads[1].wait()
    rows = pl.ds(64 * core, 64)
    for c in range(2):
        send(u_own.at[pl.ds(4 * c, 2)], u_near.at[pl.ds(0, 2), rows, :], u_sem.at[0, core], chip_u(before, c))
        send(u_own.at[pl.ds(4 * c + 2, 2)], u_near.at[pl.ds(2, 2), rows, :], u_sem.at[1, core], chip_u(after, c))
    send(u_own.at[pl.ds(4 * (1 - core), 4)], u_chip.at[:, rows, :], d2d_sem, chip_u(ring, 1 - core))

    def landed(ref, sem):
        pltpu.make_async_copy(ref, ref, sem).wait()

    loads[3].wait()
    energy_u = jnp.zeros((64, 256), F32)
    energy_v = jnp.zeros((64, 256), F32)
    for p in range(8):
        energy_u += u_own[p] * u_own[p]
        energy_v += v_own[p] * v_own[p]
    z_sums = []
    for lag in range(5):
        total = jnp.zeros((64, 256), F32)
        for p in range(8 - lag):
            total += w_own[p] * w_own[p + lag]
        z_sums.append(total)
    lane = lax.broadcasted_iota(jnp.int32, (1, 128), 1)
    scalars = jnp.zeros((1, 128), F32)
    for i, total in enumerate([energy_u, energy_v] + z_sums):
        scalars = jnp.where(lane == i, jnp.sum(total), scalars)

    v_split = split(v_own[...].reshape(512, 256))
    v_same = gram(v_split, v_split, TN)

    loads[2].wait()
    landed(u_chip.at[:, rows, :], d2d_sem)
    u_same = jnp.zeros((128, 128), F32)
    u_parts = [split(u_chip[p]) for p in range(4)]
    for p in range(4):
        u_same += gram(u_parts[p], u_parts[p], NT)

    landed(v_pair.at[0, pl.ds(0, 2)], v_sem.at[0, 0])
    send(v_pair.at[0, pl.ds(0, 2)], v_fwd.at[pl.ds(0, 2)], y_sem.at[0], place(x, (y + 3) % 4, z, core))
    landed(v_pair.at[1, pl.ds(2, 2)], v_sem.at[1, 0])
    send(v_pair.at[1, pl.ds(2, 2)], v_fwd.at[pl.ds(2, 2)], y_sem.at[1], place(x, (y + 1) % 4, z, core))

    landed(v_pair.at[0, pl.ds(2, 2)], v_sem.at[0, 1])
    landed(v_pair.at[1, pl.ds(0, 2)], v_sem.at[1, 1])
    left = split(v_pair[0].reshape(256, 256))
    right = split(v_pair[1].reshape(256, 256))
    v_cross = gram(left, right, TN)

    u_cross = jnp.zeros((128, 128), F32)
    for c in range(2):
        landed(u_near.at[pl.ds(0, 2), pl.ds(64 * c, 64), :], u_sem.at[0, c])
        landed(u_near.at[pl.ds(2, 2), pl.ds(64 * c, 64), :], u_sem.at[1, c])
    for p in range(4):
        part = split(u_near[p])
        mine = split(u_chip[p])
        u_cross += gram(mine, part, NT) if p < 2 else gram(part, mine, NT)

    landed(v_fwd.at[pl.ds(0, 2)], y_sem.at[0])
    landed(v_fwd.at[pl.ds(2, 2)], y_sem.at[1])
    first = split(v_fwd[0:2].reshape(128, 256))
    second = split(v_fwd[2:4].reshape(128, 256))
    here_right = split(v_pair[1, 0:2].reshape(128, 256))
    here_left = split(v_pair[0, 2:4].reshape(128, 256))
    v_cross += gram(here_right, first, TN)
    v_cross += gram(second, here_left, TN)

    row = lax.broadcasted_iota(jnp.int32, (128, 128), 0)
    col = lax.broadcasted_iota(jnp.int32, (128, 128), 1)
    u_block = jnp.where(col > row, u_same, u_cross)
    near = jnp.where(col > row, v_same[:128, :128] + v_same[128:, 128:], v_cross[:128, :128] + v_cross[128:, 128:])
    far = v_same[:128, 128:] + v_cross[128:, :128]
    tile[0:1] = lag_row(u_block)
    tile[1:2] = lag_row(jnp.where(col < row, far, near))
    tile[2:3] = lag_row(jnp.where(col < row, near, far))
    tile[3:4] = scalars

    def all_sum(src, got, own, group, index):
        got[own] = src[...]

        def one(i, carry):
            pltpu.make_async_remote_copy(
                src_ref=src, dst_ref=got.at[own], send_sem=red_send.at[index], recv_sem=red_recv.at[index],
                device_id=group(i), device_id_type=MESH).start()
            return carry

        lax.fori_loop(1, 16, one, 0)
        landed(got.at[pl.ds(0, 15)], red_recv.at[index])
        return jnp.sum(got[...], axis=0)

    mid[...] = all_sum(tile, got1, gx % 16, group1, 0)
    sums = all_sum(mid, got2, own2, group2, 1)

    sums = jnp.concatenate([sums, jnp.zeros((4, 128), F32)], axis=0)
    lag = lax.broadcasted_iota(jnp.int32, (128, 16), 0)

    def pick(sep):
        chosen = jnp.where(lag == sep, 1.0, 0.0).astype(F32)
        return lax.dot_general(sums, chosen, (((1,), (0,)), ((), ())),
                               precision=lax.Precision.HIGHEST, preferred_element_type=F32)

    sep_x, sep_y, sep_z = sx_ref[...], sy_ref[...], sz_ref[...]
    along_x = pick(sep_x % 128)[0:1]
    both_y = pick(sep_y % 128)
    along_y = jnp.where((sep_y >= 128) & (sep_y < 256), both_y[2:3], both_y[1:2])
    along_z = pick(sep_z + 2)[3:4]
    planes = 8.0
    out_ref[0:1] = along_x / sums[3:4, 0:1]
    out_ref[1:2] = along_y / sums[3:4, 1:2]
    out_ref[2:3] = along_z / sums[3:4, 2:3] * (planes / (planes - sep_z.astype(F32)))

    for copy in sends:
        copy.wait_send()
    landed(got1.at[pl.ds(0, 15)], red_send.at[0])
    landed(got2.at[pl.ds(0, 15)], red_send.at[1])


def local(u_field, v_field, w_field, sep_x, sep_y, sep_z):
    vmem = pl.BlockSpec(memory_space=pltpu.VMEM)
    hbm = pl.BlockSpec(memory_space=pl.ANY)
    block = (8, 64, 256)
    return pl.pallas_call(
        kernel,
        out_shape=jax.ShapeDtypeStruct((3, 16), F32),
        in_specs=[hbm] * 3 + [vmem] * 3,
        out_specs=vmem,
        scratch_shapes=[
            pltpu.VMEM(block, F32),
            pltpu.VMEM(block, F32),
            pltpu.VMEM(block, F32),
            pltpu.VMEM((4, 128, 256), F32),
            pltpu.VMEM((4, 128, 256), F32),
            pltpu.VMEM((2, 4, 64, 256), F32),
            pltpu.VMEM((4, 64, 256), F32),
            pltpu.VMEM((4, 128), F32),
            pltpu.VMEM((16, 4, 128), F32),
            pltpu.VMEM((4, 128), F32),
            pltpu.VMEM((16, 4, 128), F32),
            pltpu.SemaphoreType.DMA((4,)),
            pltpu.SemaphoreType.DMA((12,)),
            pltpu.SemaphoreType.DMA,
            pltpu.SemaphoreType.DMA((2, 2)),
            pltpu.SemaphoreType.DMA((2, 2)),
            pltpu.SemaphoreType.DMA((2,)),
            pltpu.SemaphoreType.DMA((2,)),
            pltpu.SemaphoreType.DMA((2,)),
        ],
        compiler_params=pltpu.CompilerParams(collective_id=0, has_side_effects=True),
    )(u_field, v_field, w_field, sep_x.reshape(1, 16), sep_y.reshape(1, 16), sep_z.reshape(1, 16))


def solution(mesh):
    placed = (P(None, "gx", "gy"),) * 3 + (P(),) * 3
    return jax.shard_map(local, mesh=mesh, in_specs=placed, out_specs=P(), check_vma=False)
```

```python
import functools

import jax
import jax.numpy as jnp
from jax import lax
from jax.experimental import pallas as pl
from jax.experimental.pallas import tpu as pltpu
from jax.sharding import PartitionSpec as P

F32 = jnp.float32
BF16 = jnp.bfloat16
MESH = pl.DeviceIdType.MESH
NT = (((1,), (1,)), ((), ()))
TN = (((0,), (0,)), ((), ()))


def place(x, y, z, core):
    return {"gy": y * 2 + x // 2, "gx": (x % 2) * 16 + z * 2 + core}


def split(value):
    high = value.astype(BF16)
    low = (value - high.astype(F32)).astype(BF16)
    return high, low


def gram(a, b, dims):
    dot = functools.partial(lax.dot_general, dimension_numbers=dims, preferred_element_type=F32)
    return dot(a[0], b[0]) + (dot(a[0], b[1]) + dot(a[1], b[0]))


def lag_row(block):
    total = block[0:8]
    for start in range(8, 128, 8):
        total += pltpu.roll(block[start:start + 8], 128 - start, 1)
    row = lax.broadcasted_iota(jnp.int32, (8, 128), 0)
    for bit in (1, 2, 4):
        total = jnp.where(row & bit != 0, pltpu.roll(total, 128 - bit, 1), total)
    return jnp.sum(total, axis=0, keepdims=True)


def kernel(u_hbm, v_hbm, w_hbm, sx_ref, sy_ref, sz_ref, out_ref,
           u_own, v_own, w_own, u_chip, u_near, u_extra, u_sum, v_pair, v_fwd, tile, got1, mid, got2,
           load_sem, send_sem, d2d_sem, u_sem, extra_sem, v_sem, y_sem, red_send, red_recv, token):
    gy = lax.axis_index("gy")
    gx = lax.axis_index("gx")
    y, x_hi = gy // 2, gy % 2
    x_lo, z, core = gx // 16, (gx // 2) % 8, gx % 2
    x = x_hi * 2 + x_lo
    ring = x_lo * 8 + z
    after, before = (ring + 1) % 16, (ring + 15) % 16

    def chip_u(pos, c):
        return {"gy": gy, "gx": pos * 2 + c}

    def group1(i):
        return {"gy": gy, "gx": x_lo * 16 + (gx % 16 + i) % 16}

    own2 = x * 4 + y

    def group2(i):
        other = (own2 + i) % 16
        return place(other // 4, other % 4, z, core)

    loads = [
        pltpu.make_async_copy(v_hbm, v_own, load_sem.at[0]),
        pltpu.make_async_copy(u_hbm, u_own, load_sem.at[1]),
        pltpu.make_async_copy(
            u_hbm.at[pl.ds(4 * core, 4)], u_chip.at[:, pl.ds(64 * core, 64), :], load_sem.at[2]),
        pltpu.make_async_copy(w_hbm, w_own, load_sem.at[3]),
    ]
    for load in loads:
        load.start()

    beside = [place((x + 1) % 4, y, z, core), place((x + 3) % 4, y, z, core),
              place(x, (y + 1) % 4, z, core), place(x, (y + 3) % 4, z, core),
              place(x, y, (z + 1) % 8, core), place(x, y, (z + 7) % 8, core)]
    others = [place(x, y, z, 1 - core), place(x, y, (z + 1) % 8, 1 - core), place(x, y, (z + 7) % 8, 1 - core)]
    others += [chip_u(pos, c) for pos in (after, before) for c in range(2)]
    barrier = pltpu.get_barrier_semaphore()
    for target in beside + others:
        pl.semaphore_signal(barrier, inc=1, device_id=target, device_id_type=MESH)
    pl.semaphore_wait(barrier, len(beside) + len(others))

    def tell(step):
        for target in beside:
            pl.semaphore_signal(token.at[step], inc=1, device_id=target, device_id_type=MESH)

    def told(step):
        pl.semaphore_wait(token.at[step], len(beside))

    sends = []

    def remote(src, dst, sem, target, slot):
        return pltpu.make_async_remote_copy(
            src_ref=src, dst_ref=dst, send_sem=send_sem.at[slot], recv_sem=sem,
            device_id=target, device_id_type=MESH)

    def send(*args):
        copy = remote(*args, len(sends))
        copy.start()
        sends.append(copy)

    def landed(ref, sem):
        pltpu.make_async_copy(ref, ref, sem).wait()

    first_last, last_first = z == 0, z == 7
    rows = pl.ds(64 * core, 64)

    def to_before(c, k):
        return (u_own.at[4 * c + k], u_near.at[k, rows, :], u_sem.at[0, k, core], chip_u(before, c))

    def to_after(c, k):
        return (u_own.at[4 * c + 3 - k], u_near.at[3 - k, rows, :], u_sem.at[1, k, core], chip_u(after, c))

    def to_close(c):
        return (u_own.at[4 * c + 2], u_extra.at[rows, :], extra_sem.at[core], chip_u(before, c))

    loads[0].wait()
    loads[1].wait()
    for j in range(4):
        lead = (x_hi * 2 + j) % 4
        for step in (1, 3):
            other = (x + step) % 4
            base = ((other + 3) % 4) // 2 * 4
            send(v_own.at[base + lead], v_pair.at[x_hi, lead], v_sem.at[x_hi, j], place(other, y, z, core))
        if j == 0:
            send(u_own.at[pl.ds(4 * (1 - core), 4)], u_chip.at[:, rows, :], d2d_sem, chip_u(ring, 1 - core))
        if j == 1 or j == 3:
            k = j // 2
            for c in range(2):
                send(*to_before(c, k))
                if k == 0:
                    send(*to_after(c, k))
    base_slot = len(sends) + 4
    for c in range(2):
        @pl.when(jnp.logical_not(last_first))
        def _():
            remote(*to_after(c, 1), base_slot + c).start()

        @pl.when(first_last)
        def _():
            remote(*to_close(c), base_slot + 2 + c).start()

    tell(0)

    loads[3].wait()
    energy_u = jnp.zeros((64, 256), F32)
    energy_v = jnp.zeros((64, 256), F32)
    for p in range(8):
        energy_u += u_own[p] * u_own[p]
        energy_v += v_own[p] * v_own[p]
    z_sums = []
    for lag in range(5):
        total = jnp.zeros((64, 256), F32)
        for p in range(8 - lag):
            total += w_own[p] * w_own[p + lag]
        z_sums.append(total)
    lane = lax.broadcasted_iota(jnp.int32, (1, 128), 1)
    scalars = jnp.zeros((1, 128), F32)
    for i, total in enumerate([energy_u, energy_v] + z_sums):
        scalars = jnp.where(lane == i, jnp.sum(total), scalars)
    tile[3:4] = scalars

    told(0)
    tell(1)
    v_split = split(v_own[...].reshape(512, 256))
    v_same = gram(v_split, v_split, TN)

    loads[2].wait()
    landed(u_chip.at[:, rows, :], d2d_sem)
    u_same = jnp.zeros((128, 128), F32)
    for p in range(4):
        part = split(u_chip[p])
        u_same += gram(part, part, NT)
    told(1)
    tell(2)

    for k in range(2):
        landed(v_pair.at[0, k], v_sem.at[0, k])
        send(v_pair.at[0, k], v_fwd.at[k], y_sem.at[0, k], place(x, (y + 3) % 4, z, core))
        landed(v_pair.at[1, 2 + k], v_sem.at[1, k])
        send(v_pair.at[1, 2 + k], v_fwd.at[2 + k], y_sem.at[1, k], place(x, (y + 1) % 4, z, core))

    def near_u(k):
        for c in range(2):
            half = pl.ds(64 * c, 64)
            landed(u_near.at[k, half, :], u_sem.at[0, k, c])

            def other_side():
                landed(u_near.at[3 - k, half, :], u_sem.at[1, k, c])

            if k == 0:
                other_side()
            else:
                pl.when(jnp.logical_not(first_last))(other_side)

                @pl.when(last_first)
                def _():
                    landed(u_extra.at[half, :], extra_sem.at[c])

    def cross_v(k):
        landed(v_pair.at[1, k], v_sem.at[1, 2 + k])
        landed(v_pair.at[0, 2 + k], v_sem.at[0, 2 + k])
        landed(v_fwd.at[k], y_sem.at[0, k])
        landed(v_fwd.at[2 + k], y_sem.at[1, k])
        a = [v_pair[0, k], v_pair[0, 2 + k], v_pair[1, k], v_fwd[2 + k]]
        b = [v_pair[1, k], v_pair[1, 2 + k], v_fwd[k], v_pair[0, 2 + k]]
        return gram(split(jnp.concatenate(a, axis=0)), split(jnp.concatenate(b, axis=0)), TN)

    near_u(0)
    u_sum[...] = gram(split(u_chip[0]), split(u_near[0]), NT) + gram(split(u_near[3]), split(u_chip[3]), NT)
    v_cross = cross_v(0)
    near_u(1)
    u_sum[...] += gram(split(u_chip[1]), split(u_near[1]), NT)

    @pl.when(jnp.logical_not(first_last))
    def _():
        u_sum[...] += gram(split(u_near[2]), split(u_chip[2]), NT)

    @pl.when(last_first)
    def _():
        u_sum[...] += gram(split(u_chip[2]), split(u_extra[...]), NT)

    row = lax.broadcasted_iota(jnp.int32, (128, 128), 0)
    col = lax.broadcasted_iota(jnp.int32, (128, 128), 1)
    tile[0:1] = lag_row(jnp.where(col > row, u_same, u_sum[...]))
    v_cross += cross_v(1)
    near = jnp.where(col > row, v_same[:128, :128] + v_same[128:, 128:], v_cross[:128, :128] + v_cross[128:, 128:])
    far = v_same[:128, 128:] + v_cross[128:, :128]
    tile[1:2] = lag_row(jnp.where(col < row, far, near))
    tile[2:3] = lag_row(jnp.where(col < row, near, far))
    told(2)

    def all_sum(src, got, own, group, index):
        got[own] = src[...]

        def one(i, carry):
            pltpu.make_async_remote_copy(
                src_ref=src, dst_ref=got.at[own], send_sem=red_send.at[index], recv_sem=red_recv.at[index],
                device_id=group(i), device_id_type=MESH).start()
            return carry

        lax.fori_loop(1, 16, one, 0)
        landed(got.at[pl.ds(0, 15)], red_recv.at[index])
        return jnp.sum(got[...], axis=0)

    mid[...] = all_sum(tile, got1, gx % 16, group1, 0)
    sums = all_sum(mid, got2, own2, group2, 1)

    sums = jnp.concatenate([sums, jnp.zeros((4, 128), F32)], axis=0)
    lag = lax.broadcasted_iota(jnp.int32, (128, 16), 0)

    def pick(sep):
        chosen = jnp.where(lag == sep, 1.0, 0.0).astype(F32)
        return lax.dot_general(sums, chosen, (((1,), (0,)), ((), ())),
                               precision=lax.Precision.HIGHEST, preferred_element_type=F32)

    sep_x, sep_y, sep_z = sx_ref[...], sy_ref[...], sz_ref[...]
    along_x = pick(sep_x % 128)[0:1]
    both_y = pick(sep_y % 128)
    along_y = jnp.where((sep_y >= 128) & (sep_y < 256), both_y[2:3], both_y[1:2])
    along_z = pick(sep_z + 2)[3:4]
    planes = 8.0
    out_ref[0:1] = along_x / sums[3:4, 0:1]
    out_ref[1:2] = along_y / sums[3:4, 1:2]
    out_ref[2:3] = along_z / sums[3:4, 2:3] * (planes / (planes - sep_z.astype(F32)))

    for copy in sends:
        copy.wait_send()
    for c in range(2):
        @pl.when(jnp.logical_not(last_first))
        def _():
            remote(*to_after(c, 1), base_slot + c).wait_send()

        @pl.when(first_last)
        def _():
            remote(*to_close(c), base_slot + 2 + c).wait_send()

    landed(got1.at[pl.ds(0, 15)], red_send.at[0])
    landed(got2.at[pl.ds(0, 15)], red_send.at[1])


def local(u_field, v_field, w_field, sep_x, sep_y, sep_z):
    vmem = pl.BlockSpec(memory_space=pltpu.VMEM)
    hbm = pl.BlockSpec(memory_space=pl.ANY)
    block = (8, 64, 256)
    return pl.pallas_call(
        kernel,
        out_shape=jax.ShapeDtypeStruct((3, 16), F32),
        in_specs=[hbm] * 3 + [vmem] * 3,
        out_specs=vmem,
        scratch_shapes=[
            pltpu.VMEM(block, F32),
            pltpu.VMEM(block, F32),
            pltpu.VMEM(block, F32),
            pltpu.VMEM((4, 128, 256), F32),
            pltpu.VMEM((4, 128, 256), F32),
            pltpu.VMEM((128, 256), F32),
            pltpu.VMEM((128, 128), F32),
            pltpu.VMEM((2, 4, 64, 256), F32),
            pltpu.VMEM((4, 64, 256), F32),
            pltpu.VMEM((4, 128), F32),
            pltpu.VMEM((16, 4, 128), F32),
            pltpu.VMEM((4, 128), F32),
            pltpu.VMEM((16, 4, 128), F32),
            pltpu.SemaphoreType.DMA((4,)),
            pltpu.SemaphoreType.DMA((23,)),
            pltpu.SemaphoreType.DMA,
            pltpu.SemaphoreType.DMA((2, 2, 2)),
            pltpu.SemaphoreType.DMA((2,)),
            pltpu.SemaphoreType.DMA((2, 4)),
            pltpu.SemaphoreType.DMA((2, 2)),
            pltpu.SemaphoreType.DMA((2,)),
            pltpu.SemaphoreType.DMA((2,)),
            pltpu.SemaphoreType.REGULAR((3,)),
        ],
        compiler_params=pltpu.CompilerParams(collective_id=0, has_side_effects=True),
    )(u_field, v_field, w_field, sep_x.reshape(1, 16), sep_y.reshape(1, 16), sep_z.reshape(1, 16))


def solution(mesh):
    placed = (P(None, "gx", "gy"),) * 3 + (P(),) * 3
    return jax.shard_map(local, mesh=mesh, in_specs=placed, out_specs=P(), check_vma=False)
```

```python
import functools

import jax
import jax.numpy as jnp
from jax import lax
from jax.experimental import pallas as pl
from jax.experimental.pallas import tpu as pltpu
from jax.sharding import PartitionSpec as P

F32 = jnp.float32
BF16 = jnp.bfloat16
MESH = pl.DeviceIdType.MESH
NT = (((1,), (1,)), ((), ()))
TN = (((0,), (0,)), ((), ()))


def place(x, y, z, core):
    return {"gy": y * 2 + x // 2, "gx": (x % 2) * 16 + z * 2 + core}


def split(value):
    high = value.astype(BF16)
    low = (value - high.astype(F32)).astype(BF16)
    return high, low


def gram(a, b, dims):
    dot = functools.partial(lax.dot_general, dimension_numbers=dims, preferred_element_type=F32)
    return dot(a[0], b[0]) + (dot(a[0], b[1]) + dot(a[1], b[0]))


def lag_row(block):
    total = block[0:8]
    for start in range(8, 128, 8):
        total += pltpu.roll(block[start:start + 8], 128 - start, 1)
    row = lax.broadcasted_iota(jnp.int32, (8, 128), 0)
    for bit in (1, 2, 4):
        total = jnp.where(row & bit != 0, pltpu.roll(total, 128 - bit, 1), total)
    return jnp.sum(total, axis=0, keepdims=True)


def kernel(u_hbm, v_hbm, w_hbm, sx_hbm, sy_hbm, sz_hbm, out_ref,
           u_own, v_own, w_own, u_chip, u_near, u_extra, u_hand, u_sum, v_pair, v_fwd, tile, got1, mid, got2,
           load_sem, send_sem, d2d_sem, u_sem, extra_sem, hand_sem, v_sem, y_sem, red_send, red_recv, token, back, sx_ref, sy_ref, sz_ref, sep_sem):
    gy = lax.axis_index("gy")
    gx = lax.axis_index("gx")
    y, x_hi = gy // 2, gy % 2
    x_lo, z, core = gx // 16, (gx // 2) % 8, gx % 2
    x = x_hi * 2 + x_lo
    ring = x_lo * 8 + z
    after, before = (ring + 1) % 16, (ring + 15) % 16

    def chip_u(pos, c):
        return {"gy": gy, "gx": pos * 2 + c}

    def group1(i):
        return {"gy": gy, "gx": x_lo * 16 + (gx % 16 + i) % 16}

    own2 = x * 4 + y

    def group2(i):
        other = (own2 + i) % 16
        return place(other // 4, other % 4, z, core)

    loads = [
        pltpu.make_async_copy(v_hbm, v_own, load_sem.at[0]),
        pltpu.make_async_copy(u_hbm, u_own, load_sem.at[1]),
        pltpu.make_async_copy(
            u_hbm.at[pl.ds(4 * core, 4)], u_chip.at[:, pl.ds(64 * core, 64), :], load_sem.at[2]),
        pltpu.make_async_copy(w_hbm, w_own, load_sem.at[3]),
    ]
    for load in loads:
        load.start()
    lags = [pltpu.make_async_copy(src, dst, sep_sem.at[i])
            for i, (src, dst) in enumerate([(sx_hbm, sx_ref), (sy_hbm, sy_ref), (sz_hbm, sz_ref)])]
    for load in lags:
        load.start()

    first, second, last = z == 0, z == 1, z == 7
    in_plane = [place((x + 1) % 4, y, z, core), place((x + 3) % 4, y, z, core),
                place(x, (y + 1) % 4, z, core), place(x, (y + 3) % 4, z, core), chip_u(ring, 1 - core)]
    beside = in_plane[:4] + [place(x, y, (z + 1) % 8, core), place(x, y, (z + 7) % 8, core)]
    wrapped = [chip_u(x_lo * 8 + 7 - z, c) for c in range(2)]
    two_back = [chip_u((ring + 14) % 16, c) for c in range(2)]
    two_on = [chip_u((ring + 2) % 16, c) for c in range(2)]
    chip_before = [chip_u(before, c) for c in range(2)]
    chip_after = [chip_u(after, c) for c in range(2)]
    across = chip_u((ring + 8) % 16, core)

    def signal(sem, targets):
        for target in targets:
            pl.semaphore_signal(sem, inc=1, device_id=target, device_id_type=MESH)

    barrier = pltpu.get_barrier_semaphore()
    signal(barrier, in_plane)

    @pl.when(jnp.logical_not(last))
    def _():
        signal(barrier, chip_after)

    @pl.when(first)
    def _():
        signal(barrier, wrapped)

    @pl.when(second)
    def _():
        signal(barrier, two_back)

    pl.semaphore_wait(barrier, 5 + 2 * jnp.minimum(z, 1) + 4 * (z // 7))

    def tell(step):
        signal(token.at[step], beside)

    def told(step):
        pl.semaphore_wait(token.at[step], len(beside))

    sends = []

    def remote(src, dst, sem, target, slot):
        return pltpu.make_async_remote_copy(
            src_ref=src, dst_ref=dst, send_sem=send_sem.at[slot], recv_sem=sem,
            device_id=target, device_id_type=MESH)

    def send(*args):
        copy = remote(*args, len(sends))
        copy.start()
        sends.append(copy)

    def landed(ref, sem):
        pltpu.make_async_copy(ref, ref, sem).wait()

    rows = pl.ds(64 * core, 64)
    pieces = [(k, c) for k in range(2) for c in range(2)]

    def to_before(k, c):
        return (u_own.at[4 * c + k], u_near.at[k, rows, :], u_sem.at[0, k, core], chip_before[c], 13 + 2 * k + c)

    def to_after(k, c):
        return (u_own.at[4 * c + 3 - k], u_near.at[3 - k, rows, :], u_sem.at[1, k, core], chip_after[c], 17 + 2 * k + c)

    def to_across(k, c):
        return (u_own.at[4 * c + k], u_hand.at[k, c], hand_sem.at[k, c], across, 13 + 2 * k + c)

    def hand_on(k, c):
        return (u_hand.at[k, c], u_near.at[k, rows, :], u_sem.at[0, k, core], wrapped[c], 21 + 2 * k + c)

    def to_second(k, c):
        return (u_own.at[4 * c + 3 - k], u_extra.at[1 - k, rows, :], extra_sem.at[k, core], two_on[c], 17 + 2 * k + c)

    loads[1].wait()

    @pl.when(first)
    def _():
        for piece in pieces:
            remote(*to_across(*piece)).start()

    @pl.when(jnp.logical_not(first))
    def _():
        for piece in pieces:
            remote(*to_before(*piece)).start()
        signal(back, chip_before)

    @pl.when(last)
    def _():
        for piece in pieces:
            remote(*to_second(*piece)).start()
        signal(back, wrapped)

    loads[0].wait()
    for j in range(4):
        lead = (x_hi * 2 + j) % 4
        for step in (1, 3):
            other = (x + step) % 4
            base = ((other + 3) % 4) // 2 * 4
            send(v_own.at[base + lead], v_pair.at[x_hi, lead], v_sem.at[x_hi, j], place(other, y, z, core))
    send(u_own.at[pl.ds(4 * (1 - core), 4)], u_chip.at[:, rows, :], d2d_sem, chip_u(ring, 1 - core))

    loads[3].wait()
    energy_u = jnp.zeros((64, 256), F32)
    energy_v = jnp.zeros((64, 256), F32)
    for p in range(8):
        energy_u += u_own[p] * u_own[p]
        energy_v += v_own[p] * v_own[p]
    z_sums = []
    for lag in range(5):
        total = jnp.zeros((64, 256), F32)
        for p in range(8 - lag):
            total += w_own[p] * w_own[p + lag]
        z_sums.append(total)
    lane = lax.broadcasted_iota(jnp.int32, (1, 128), 1)
    scalars = jnp.zeros((1, 128), F32)
    for i, total in enumerate([energy_u, energy_v] + z_sums):
        scalars = jnp.where(lane == i, jnp.sum(total), scalars)
    tile[3:4] = scalars

    @pl.when(jnp.logical_not(last))
    def _():
        pl.semaphore_wait(back, 2 + 2 * (1 - jnp.minimum(z, 1)))
        for piece in pieces:
            remote(*to_after(*piece)).start()

    @pl.when(first)
    def _():
        for k, c in pieces:
            landed(u_hand.at[k, c], hand_sem.at[k, c])
            remote(*hand_on(k, c)).start()

    tell(0)

    v_split = split(v_own[...].reshape(512, 256))
    v_same = gram(v_split, v_split, TN)

    loads[2].wait()
    landed(u_chip.at[:, rows, :], d2d_sem)
    u_same = jnp.zeros((128, 128), F32)
    for p in range(4):
        part = split(u_chip[p])
        u_same += gram(part, part, NT)

    def pass_on(k):
        landed(v_pair.at[0, k], v_sem.at[0, k])
        send(v_pair.at[0, k], v_fwd.at[k], y_sem.at[0, k], place(x, (y + 3) % 4, z, core))
        landed(v_pair.at[1, 2 + k], v_sem.at[1, k])
        send(v_pair.at[1, 2 + k], v_fwd.at[2 + k], y_sem.at[1, k], place(x, (y + 1) % 4, z, core))

    def near_u(k):
        for c in range(2):
            landed(u_near.at[k, pl.ds(64 * c, 64), :], u_sem.at[0, k, c])
        term = gram(split(u_chip[k]), split(u_near[k]), NT)
        if k == 0:
            u_sum[...] = term
        else:
            u_sum[...] += term

        @pl.when(jnp.logical_not(first))
        def _():
            for c in range(2):
                landed(u_near.at[3 - k, pl.ds(64 * c, 64), :], u_sem.at[1, k, c])
            u_sum[...] += gram(split(u_near[3 - k]), split(u_chip[3 - k]), NT)

    def cross_v(k):
        landed(v_pair.at[1, k], v_sem.at[1, 2 + k])
        landed(v_pair.at[0, 2 + k], v_sem.at[0, 2 + k])
        landed(v_fwd.at[k], y_sem.at[0, k])
        landed(v_fwd.at[2 + k], y_sem.at[1, k])
        a = [v_pair[0, k], v_pair[0, 2 + k], v_pair[1, k], v_fwd[2 + k]]
        b = [v_pair[1, k], v_pair[1, 2 + k], v_fwd[k], v_pair[0, 2 + k]]
        return gram(split(jnp.concatenate(a, axis=0)), split(jnp.concatenate(b, axis=0)), TN)

    pass_on(0)
    told(0)
    tell(1)
    pass_on(1)
    near_u(0)
    told(1)
    tell(2)
    v_cross = cross_v(0)
    near_u(1)
    @pl.when(second)
    def _():
        for k in range(2):
            for c in range(2):
                landed(u_extra.at[1 - k, pl.ds(64 * c, 64), :], extra_sem.at[k, c])
            u_sum[...] += gram(split(u_extra[1 - k]), split(u_near[3 - k]), NT)

    row = lax.broadcasted_iota(jnp.int32, (128, 128), 0)
    col = lax.broadcasted_iota(jnp.int32, (128, 128), 1)
    tile[0:1] = lag_row(jnp.where(col > row, u_same, u_sum[...]))
    v_cross += cross_v(1)
    near = jnp.where(col > row, v_same[:128, :128] + v_same[128:, 128:], v_cross[:128, :128] + v_cross[128:, 128:])
    far = v_same[:128, 128:] + v_cross[128:, :128]
    tile[1:2] = lag_row(jnp.where(col < row, far, near))
    tile[2:3] = lag_row(jnp.where(col < row, near, far))
    told(2)
    for load in lags:
        load.wait()

    def all_sum(src, got, own, group, index):
        got[own] = src[...]

        def one(i, carry):
            pltpu.make_async_remote_copy(
                src_ref=src, dst_ref=got.at[own], send_sem=red_send.at[index], recv_sem=red_recv.at[index],
                device_id=group(i), device_id_type=MESH).start()
            return carry

        lax.fori_loop(1, 16, one, 0)
        landed(got.at[pl.ds(0, 15)], red_recv.at[index])
        return jnp.sum(got[...], axis=0)

    mid[...] = all_sum(tile, got1, gx % 16, group1, 0)
    sums = all_sum(mid, got2, own2, group2, 1)

    sums = jnp.concatenate([sums, jnp.zeros((4, 128), F32)], axis=0)
    lag = lax.broadcasted_iota(jnp.int32, (128, 16), 0)

    def pick(sep):
        chosen = jnp.where(lag == sep, 1.0, 0.0).astype(F32)
        return lax.dot_general(sums, chosen, (((1,), (0,)), ((), ())),
                               precision=lax.Precision.HIGHEST, preferred_element_type=F32)

    sep_x, sep_y, sep_z = sx_ref[...], sy_ref[...], sz_ref[...]
    along_x = pick(sep_x % 128)[0:1]
    both_y = pick(sep_y % 128)
    along_y = jnp.where((sep_y >= 128) & (sep_y < 256), both_y[2:3], both_y[1:2])
    along_z = pick(sep_z + 2)[3:4]
    planes = 8.0
    out_ref[0:1] = along_x / sums[3:4, 0:1]
    out_ref[1:2] = along_y / sums[3:4, 1:2]
    out_ref[2:3] = along_z / sums[3:4, 2:3] * (planes / (planes - sep_z.astype(F32)))

    for copy in sends:
        copy.wait_send()
    for piece in pieces:
        remote(*to_before(*piece)).wait_send()
        remote(*to_after(*piece)).wait_send()

        @pl.when(first)
        def _():
            remote(*hand_on(*piece)).wait_send()

    landed(got1.at[pl.ds(0, 15)], red_send.at[0])
    landed(got2.at[pl.ds(0, 15)], red_send.at[1])


def local(u_field, v_field, w_field, sep_x, sep_y, sep_z):
    vmem = pl.BlockSpec(memory_space=pltpu.VMEM)
    hbm = pl.BlockSpec(memory_space=pl.ANY)
    block = (8, 64, 256)
    return pl.pallas_call(
        kernel,
        out_shape=pltpu.VMEM((3, 16), F32),
        in_specs=[hbm] * 6,
        out_specs=vmem,
        scratch_shapes=[
            pltpu.VMEM(block, F32),
            pltpu.VMEM(block, F32),
            pltpu.VMEM(block, F32),
            pltpu.VMEM((4, 128, 256), F32),
            pltpu.VMEM((4, 128, 256), F32),
            pltpu.VMEM((2, 128, 256), F32),
            pltpu.VMEM((2, 2, 64, 256), F32),
            pltpu.VMEM((128, 128), F32),
            pltpu.VMEM((2, 4, 64, 256), F32),
            pltpu.VMEM((4, 64, 256), F32),
            pltpu.VMEM((4, 128), F32),
            pltpu.VMEM((16, 4, 128), F32),
            pltpu.VMEM((4, 128), F32),
            pltpu.VMEM((16, 4, 128), F32),
            pltpu.SemaphoreType.DMA((4,)),
            pltpu.SemaphoreType.DMA((25,)),
            pltpu.SemaphoreType.DMA,
            pltpu.SemaphoreType.DMA((2, 2, 2)),
            pltpu.SemaphoreType.DMA((2, 2)),
            pltpu.SemaphoreType.DMA((2, 2)),
            pltpu.SemaphoreType.DMA((2, 4)),
            pltpu.SemaphoreType.DMA((2, 2)),
            pltpu.SemaphoreType.DMA((2,)),
            pltpu.SemaphoreType.DMA((2,)),
            pltpu.SemaphoreType.REGULAR((3,)),
            pltpu.SemaphoreType.REGULAR,
            pltpu.VMEM((1, 16), jnp.int32),
            pltpu.VMEM((1, 16), jnp.int32),
            pltpu.VMEM((1, 16), jnp.int32),
            pltpu.SemaphoreType.DMA((3,)),
        ],
        compiler_params=pltpu.CompilerParams(collective_id=0, has_side_effects=True),
    )(u_field, v_field, w_field, sep_x.reshape(1, 16), sep_y.reshape(1, 16), sep_z.reshape(1, 16))


def solution(mesh):
    placed = (P(None, "gx", "gy"),) * 3 + (P(),) * 3
    return jax.shard_map(local, mesh=mesh, in_specs=placed, out_specs=P(), check_vma=False)
```

```python
import functools

import jax
import jax.numpy as jnp
from jax import lax
from jax.experimental import pallas as pl
from jax.experimental.pallas import tpu as pltpu
from jax.sharding import PartitionSpec as P

F32 = jnp.float32
BF16 = jnp.bfloat16
MESH = pl.DeviceIdType.MESH
NT = (((1,), (1,)), ((), ()))
TN = (((0,), (0,)), ((), ()))


def place(x, y, z, core):
    return {"gy": y * 2 + x // 2, "gx": (x % 2) * 16 + z * 2 + core}


def split(value):
    high = value.astype(BF16)
    low = (value - high.astype(F32)).astype(BF16)
    return high, low


def gram(a, b, dims):
    dot = functools.partial(lax.dot_general, dimension_numbers=dims, preferred_element_type=F32)
    return dot(a[0], b[0]) + (dot(a[0], b[1]) + dot(a[1], b[0]))


def lag_row(block):
    total = block[0:8]
    for start in range(8, 128, 8):
        total += pltpu.roll(block[start:start + 8], 128 - start, 1)
    row = lax.broadcasted_iota(jnp.int32, (8, 128), 0)
    for bit in (1, 2, 4):
        total = jnp.where(row & bit != 0, pltpu.roll(total, 128 - bit, 1), total)
    return jnp.sum(total, axis=0, keepdims=True)


def kernel(u_hbm, v_hbm, w_hbm, sx_hbm, sy_hbm, sz_hbm, out_ref,
           u_own, v_own, w_own, u_chip, u_near, u_extra, u_hand, u_sum, v_pair, v_fwd, tile, got1, mid, got2,
           load_sem, send_sem, d2d_sem, u_sem, extra_sem, hand_sem, v_sem, y_sem, red_send, red_recv, token, back, wrap_back, sx_ref, sy_ref, sz_ref, sep_sem):
    gy = lax.axis_index("gy")
    gx = lax.axis_index("gx")
    y, x_hi = gy // 2, gy % 2
    x_lo, z, core = gx // 16, (gx // 2) % 8, gx % 2
    x = x_hi * 2 + x_lo
    ring = x_lo * 8 + z
    after, before = (ring + 1) % 16, (ring + 15) % 16

    def chip_u(pos, c):
        return {"gy": gy, "gx": pos * 2 + c}

    def group1(i):
        return {"gy": gy, "gx": x_lo * 16 + (gx % 16 + i) % 16}

    own2 = x * 4 + y

    def group2(i):
        other = (own2 + i) % 16
        return place(other // 4, other % 4, z, core)

    loads = [
        pltpu.make_async_copy(v_hbm, v_own, load_sem.at[0]),
        pltpu.make_async_copy(u_hbm, u_own, load_sem.at[1]),
        pltpu.make_async_copy(
            u_hbm.at[pl.ds(4 * core, 4)], u_chip.at[:, pl.ds(64 * core, 64), :], load_sem.at[2]),
        pltpu.make_async_copy(w_hbm, w_own, load_sem.at[3]),
    ]
    for load in loads:
        load.start()
    lags = [pltpu.make_async_copy(src, dst, sep_sem.at[i])
            for i, (src, dst) in enumerate([(sx_hbm, sx_ref), (sy_hbm, sy_ref), (sz_hbm, sz_ref)])]
    for load in lags:
        load.start()

    first, second, last = z == 0, z == 1, z == 7
    in_plane = [place((x + 1) % 4, y, z, core), place((x + 3) % 4, y, z, core),
                place(x, (y + 1) % 4, z, core), place(x, (y + 3) % 4, z, core), chip_u(ring, 1 - core)]
    beside = in_plane[:4] + [place(x, y, (z + 1) % 8, core), place(x, y, (z + 7) % 8, core)]
    wrapped = [chip_u(x_lo * 8 + 7 - z, c) for c in range(2)]
    two_back = [chip_u((ring + 14) % 16, c) for c in range(2)]
    two_on = [chip_u((ring + 2) % 16, c) for c in range(2)]
    chip_before = [chip_u(before, c) for c in range(2)]
    chip_after = [chip_u(after, c) for c in range(2)]
    across = chip_u((ring + 8) % 16, core)

    def signal(sem, targets):
        for target in targets:
            pl.semaphore_signal(sem, inc=1, device_id=target, device_id_type=MESH)

    barrier = pltpu.get_barrier_semaphore()
    signal(barrier, in_plane)

    @pl.when(jnp.logical_not(last))
    def _():
        signal(barrier, chip_after)

    @pl.when(first)
    def _():
        signal(barrier, wrapped)

    @pl.when(second)
    def _():
        signal(barrier, two_back)

    pl.semaphore_wait(barrier, 5 + 2 * jnp.minimum(z, 1) + 4 * (z // 7))

    def tell(step):
        signal(token.at[step], beside)

    def told(step):
        pl.semaphore_wait(token.at[step], len(beside))

    sends = []

    def remote(src, dst, sem, target, slot):
        return pltpu.make_async_remote_copy(
            src_ref=src, dst_ref=dst, send_sem=send_sem.at[slot], recv_sem=sem,
            device_id=target, device_id_type=MESH)

    def send(*args):
        copy = remote(*args, len(sends))
        copy.start()
        sends.append(copy)

    def landed(ref, sem):
        pltpu.make_async_copy(ref, ref, sem).wait()

    rows = pl.ds(64 * core, 64)
    pieces = [(k, c) for k in range(2) for c in range(2)]

    def to_before(k, c):
        return (u_own.at[4 * c + k], u_near.at[k, rows, :], u_sem.at[0, k, core], chip_before[c], 13 + 2 * k + c)

    def to_after(k, c):
        return (u_own.at[4 * c + 3 - k], u_near.at[3 - k, rows, :], u_sem.at[1, k, core], chip_after[c], 17 + 2 * k + c)

    def to_across(k, c):
        return (u_own.at[4 * c + k], u_hand.at[k, c], hand_sem.at[k, c], across, 13 + 2 * k + c)

    def hand_on(k, c):
        return (u_hand.at[k, c], u_near.at[k, rows, :], u_sem.at[0, k, core], wrapped[c], 21 + 2 * k + c)

    def to_second(k, c):
        return (u_own.at[4 * c + 3 - k], u_extra.at[1 - k, rows, :], extra_sem.at[k, core], two_on[c], 17 + 2 * k + c)

    @pl.when(jnp.logical_not(first))
    def _():
        signal(back, chip_before)

    @pl.when(last)
    def _():
        signal(wrap_back, wrapped)

    loads[1].wait()

    @pl.when(first)
    def _():
        for piece in pieces:
            remote(*to_across(*piece)).start()

    @pl.when(jnp.logical_not(first))
    def _():
        for piece in pieces:
            remote(*to_before(*piece)).start()

    @pl.when(last)
    def _():
        for piece in pieces:
            remote(*to_second(*piece)).start()

    loads[0].wait()
    for j in range(4):
        lead = (x_hi * 2 + j) % 4
        for step in (1, 3):
            other = (x + step) % 4
            base = ((other + 3) % 4) // 2 * 4
            send(v_own.at[base + lead], v_pair.at[x_hi, lead], v_sem.at[x_hi, j], place(other, y, z, core))
    send(u_own.at[pl.ds(4 * (1 - core), 4)], u_chip.at[:, rows, :], d2d_sem, chip_u(ring, 1 - core))

    loads[3].wait()
    energy_u = jnp.zeros((64, 256), F32)
    energy_v = jnp.zeros((64, 256), F32)
    for p in range(8):
        energy_u += u_own[p] * u_own[p]
        energy_v += v_own[p] * v_own[p]
    z_sums = []
    for lag in range(5):
        total = jnp.zeros((64, 256), F32)
        for p in range(8 - lag):
            total += w_own[p] * w_own[p + lag]
        z_sums.append(total)
    lane = lax.broadcasted_iota(jnp.int32, (1, 128), 1)
    scalars = jnp.zeros((1, 128), F32)
    for i, total in enumerate([energy_u, energy_v] + z_sums):
        scalars = jnp.where(lane == i, jnp.sum(total), scalars)
    tile[3:4] = scalars

    @pl.when(jnp.logical_not(last))
    def _():
        pl.semaphore_wait(back, 2)
        for piece in pieces:
            remote(*to_after(*piece)).start()

    @pl.when(first)
    def _():
        pl.semaphore_wait(wrap_back, 2)

    tell(0)

    @pl.when(first)
    def _():
        for k, c in pieces:
            landed(u_hand.at[k, c], hand_sem.at[k, c])
            remote(*hand_on(k, c)).start()

    v_split = split(v_own[...].reshape(512, 256))
    v_same = gram(v_split, v_split, TN)

    loads[2].wait()
    landed(u_chip.at[:, rows, :], d2d_sem)
    u_same = jnp.zeros((128, 128), F32)
    for p in range(4):
        part = split(u_chip[p])
        u_same += gram(part, part, NT)

    def pass_on(k):
        landed(v_pair.at[0, k], v_sem.at[0, k])
        send(v_pair.at[0, k], v_fwd.at[k], y_sem.at[0, k], place(x, (y + 3) % 4, z, core))
        landed(v_pair.at[1, 2 + k], v_sem.at[1, k])
        send(v_pair.at[1, 2 + k], v_fwd.at[2 + k], y_sem.at[1, k], place(x, (y + 1) % 4, z, core))

    def near_u(k):
        for c in range(2):
            landed(u_near.at[k, pl.ds(64 * c, 64), :], u_sem.at[0, k, c])
        term = gram(split(u_chip[k]), split(u_near[k]), NT)
        if k == 0:
            u_sum[...] = term
        else:
            u_sum[...] += term

        @pl.when(jnp.logical_not(first))
        def _():
            for c in range(2):
                landed(u_near.at[3 - k, pl.ds(64 * c, 64), :], u_sem.at[1, k, c])
            u_sum[...] += gram(split(u_near[3 - k]), split(u_chip[3 - k]), NT)

    def cross_v(k):
        landed(v_pair.at[1, k], v_sem.at[1, 2 + k])
        landed(v_pair.at[0, 2 + k], v_sem.at[0, 2 + k])
        landed(v_fwd.at[k], y_sem.at[0, k])
        landed(v_fwd.at[2 + k], y_sem.at[1, k])
        a = [v_pair[0, k], v_pair[0, 2 + k], v_pair[1, k], v_fwd[2 + k]]
        b = [v_pair[1, k], v_pair[1, 2 + k], v_fwd[k], v_pair[0, 2 + k]]
        return gram(split(jnp.concatenate(a, axis=0)), split(jnp.concatenate(b, axis=0)), TN)

    pass_on(0)
    told(0)
    tell(1)
    pass_on(1)
    near_u(0)
    told(1)
    tell(2)
    v_cross = cross_v(0)
    near_u(1)
    @pl.when(second)
    def _():
        for k in range(2):
            for c in range(2):
                landed(u_extra.at[1 - k, pl.ds(64 * c, 64), :], extra_sem.at[k, c])
            u_sum[...] += gram(split(u_extra[1 - k]), split(u_near[3 - k]), NT)

    row = lax.broadcasted_iota(jnp.int32, (128, 128), 0)
    col = lax.broadcasted_iota(jnp.int32, (128, 128), 1)
    tile[0:1] = lag_row(jnp.where(col > row, u_same, u_sum[...]))
    v_cross += cross_v(1)
    near = jnp.where(col > row, v_same[:128, :128] + v_same[128:, 128:], v_cross[:128, :128] + v_cross[128:, 128:])
    far = v_same[:128, 128:] + v_cross[128:, :128]
    tile[1:2] = lag_row(jnp.where(col < row, far, near))
    tile[2:3] = lag_row(jnp.where(col < row, near, far))
    told(2)
    for load in lags:
        load.wait()

    def all_sum(src, got, own, group, index):
        got[own] = src[...]

        def one(i, carry):
            pltpu.make_async_remote_copy(
                src_ref=src, dst_ref=got.at[own], send_sem=red_send.at[index], recv_sem=red_recv.at[index],
                device_id=group(i), device_id_type=MESH).start()
            return carry

        lax.fori_loop(1, 16, one, 0)
        landed(got.at[pl.ds(0, 15)], red_recv.at[index])
        return jnp.sum(got[...], axis=0)

    mid[...] = all_sum(tile, got1, gx % 16, group1, 0)
    sums = all_sum(mid, got2, own2, group2, 1)

    sums = jnp.concatenate([sums, jnp.zeros((4, 128), F32)], axis=0)
    lag = lax.broadcasted_iota(jnp.int32, (128, 16), 0)

    def pick(sep):
        chosen = jnp.where(lag == sep, 1.0, 0.0).astype(F32)
        return lax.dot_general(sums, chosen, (((1,), (0,)), ((), ())),
                               precision=lax.Precision.HIGHEST, preferred_element_type=F32)

    sep_x, sep_y, sep_z = sx_ref[...], sy_ref[...], sz_ref[...]
    along_x = pick(sep_x % 128)[0:1]
    both_y = pick(sep_y % 128)
    along_y = jnp.where((sep_y >= 128) & (sep_y < 256), both_y[2:3], both_y[1:2])
    along_z = pick(sep_z + 2)[3:4]
    planes = 8.0
    out_ref[0:1] = along_x / sums[3:4, 0:1]
    out_ref[1:2] = along_y / sums[3:4, 1:2]
    out_ref[2:3] = along_z / sums[3:4, 2:3] * (planes / (planes - sep_z.astype(F32)))

    for copy in sends:
        copy.wait_send()
    for piece in pieces:
        remote(*to_before(*piece)).wait_send()
        remote(*to_after(*piece)).wait_send()

        @pl.when(first)
        def _():
            remote(*hand_on(*piece)).wait_send()

    landed(got1.at[pl.ds(0, 15)], red_send.at[0])
    landed(got2.at[pl.ds(0, 15)], red_send.at[1])


def local(u_field, v_field, w_field, sep_x, sep_y, sep_z):
    vmem = pl.BlockSpec(memory_space=pltpu.VMEM)
    hbm = pl.BlockSpec(memory_space=pl.ANY)
    block = (8, 64, 256)
    return pl.pallas_call(
        kernel,
        out_shape=pltpu.VMEM((3, 16), F32),
        in_specs=[hbm] * 6,
        out_specs=vmem,
        scratch_shapes=[
            pltpu.VMEM(block, F32),
            pltpu.VMEM(block, F32),
            pltpu.VMEM(block, F32),
            pltpu.VMEM((4, 128, 256), F32),
            pltpu.VMEM((4, 128, 256), F32),
            pltpu.VMEM((2, 128, 256), F32),
            pltpu.VMEM((2, 2, 64, 256), F32),
            pltpu.VMEM((128, 128), F32),
            pltpu.VMEM((2, 4, 64, 256), F32),
            pltpu.VMEM((4, 64, 256), F32),
            pltpu.VMEM((4, 128), F32),
            pltpu.VMEM((16, 4, 128), F32),
            pltpu.VMEM((4, 128), F32),
            pltpu.VMEM((16, 4, 128), F32),
            pltpu.SemaphoreType.DMA((4,)),
            pltpu.SemaphoreType.DMA((25,)),
            pltpu.SemaphoreType.DMA,
            pltpu.SemaphoreType.DMA((2, 2, 2)),
            pltpu.SemaphoreType.DMA((2, 2)),
            pltpu.SemaphoreType.DMA((2, 2)),
            pltpu.SemaphoreType.DMA((2, 4)),
            pltpu.SemaphoreType.DMA((2, 2)),
            pltpu.SemaphoreType.DMA((2,)),
            pltpu.SemaphoreType.DMA((2,)),
            pltpu.SemaphoreType.REGULAR((3,)),
            pltpu.SemaphoreType.REGULAR,
            pltpu.SemaphoreType.REGULAR,
            pltpu.VMEM((1, 16), jnp.int32),
            pltpu.VMEM((1, 16), jnp.int32),
            pltpu.VMEM((1, 16), jnp.int32),
            pltpu.SemaphoreType.DMA((3,)),
        ],
        compiler_params=pltpu.CompilerParams(collective_id=0, has_side_effects=True),
    )(u_field, v_field, w_field, sep_x.reshape(1, 16), sep_y.reshape(1, 16), sep_z.reshape(1, 16))


def solution(mesh):
    placed = (P(None, "gx", "gy"),) * 3 + (P(),) * 3
    return jax.shard_map(local, mesh=mesh, in_specs=placed, out_specs=P(), check_vma=False)
```
